32 devices in a mesh: pole: 4 (over y, core), row: 2 (over x), col: 4 (over z).
Axes of the slice: x: 2, y: 2, z: 4, core: 2. Of those that a mesh axis runs over, the one named last changes fastest.
Arguments:
- l_factor: float32 [4, 2, 6, 512, 6, 512], P('pole', None, None, 'row', None, 'col'), may hold values from -0.21875 to 0.21875
- dinv: float32 [4, 2, 6, 512, 512], P('pole', None, None, 'row', 'col'), may hold values from -8 to 8, as said below
- weights: float32 [4, 2], P('pole'), may hold values from -4 to 4
- tiles: int32 [6, 24], replicated, may hold values 0 or 1
Outputs:
- density: float32 [6, 2, 256, 6, 512], P(None, 'row', 'pole', None, 'col')
The draws below stay inside these ranges and needn't reach their ends.
Inputs may be any that keep to these rules, and one draw needn't show every extreme that they name: Each of dinv's blocks is a symmetric complex matrix.
All inputs are finite; a program needn't handle non-finite values.
Results may differ from the reference program's by a relative error of at most 0.00012.
Values sent between devices are 32-bit elements; how exact they have to be, the bound alone decides.
A program may use at most 192 MiB of HBM per device.

```python
import jax
import jax.numpy as jnp
from jax import lax

W = 512
NS = 6
TILE = 128
POLES = 4
N_ROW = 2


def draw_dinv(key, part):
    first, second, third = jax.random.split(jax.random.fold_in(key, 17), 3)
    noise = jax.random.normal(first, (POLES, 2, NS, W, W), jnp.float32)
    sym = (noise + jnp.swapaxes(noise, 3, 4)) * (0.6 / (2.0 * W) ** 0.5)
    real_diag = jax.random.uniform(second, (POLES, NS, W), jnp.float32, 0.5, 1.5)
    imag_diag = jax.random.uniform(third, (POLES, NS, W), jnp.float32, -0.5, 0.5)
    eye = jnp.eye(W, dtype=jnp.float32)
    diag = jnp.stack([real_diag, imag_diag], axis=1)[..., None] * eye
    result = sym + diag
    return jnp.clip(result, -8.0, 8.0)


def touch_ends(values, stream_key, least, high):
    longest = values.shape.index(max(values.shape))
    spots = []
    for shift in (0, 1):
        where = [jax.random.randint(jax.random.fold_in(stream_key, axis), (), 0, length) for axis, length in enumerate(values.shape)]
        where[longest] = (where[longest] + shift) % values.shape[longest]
        spots.append(tuple(where))
    return values.at[spots[0]].set(least).at[spots[1]].set(high)


def steps_of(key, shape, shards, least, largest):
    level = 1.0
    for dim, blocks in shards:
        steps = jax.random.uniform(jax.random.fold_in(jax.random.fold_in(key, 6), dim), (blocks,), jnp.float32, least / len(shards), largest / len(shards))
        level = level * jnp.repeat(jnp.exp(steps), shape[dim] // blocks).reshape((-1,) + (1,) * (len(shape) - 1 - dim))
    return level


def centred(key, shape, deviation, limit, pieces=(), held_as=jnp.bfloat16):
    values = jax.random.normal(key, shape, jnp.float32) * deviation
    if len(pieces) > 0:
        values = steps_of(key, shape, pieces, -0.22, 0.18) * values
    return jnp.clip(values, min=-limit, max=limit).astype(held_as)


def setup_inputs(seed: int = 0) -> dict:
    streams_of = jax.random.split(jax.random.key(seed), 5)
    return {
        "l_factor": centred(streams_of[0], (POLES, 2, NS, W, NS, W), (NS * W // 4) ** -0.5, 0.21875, ((0, 4), (3, 2), (5, 4)), jnp.float32),
        "dinv": draw_dinv(jax.random.fold_in(streams_of[4], 71), 0),
        "weights": centred(streams_of[2], (POLES, 2), 1.0, 4.0, ((0, 4),), jnp.float32),
        "tiles": touch_ends((jax.random.randint(streams_of[3], (NS, NS * W // TILE), 0, 4) < 3).astype(jnp.int32), jax.random.fold_in(streams_of[3], 1), 0, 1),
    }


def cdot_t(left, right):
    dims = (((0,), (0,)), ((), ()))

    def single(first, second):
        return lax.dot_general(first, second, dims, precision=lax.Precision.HIGHEST, preferred_element_type=jnp.float32)

    real = single(left[0], right[0]) - single(left[1], right[1])
    imag = single(left[0], right[1]) + single(left[1], right[0])
    return jnp.stack([real, imag])


def reference(l_factor, dinv, weights, tiles):
    total = NS * W
    row_keep = jnp.repeat(tiles, TILE, axis=1)
    keep = jnp.repeat(row_keep, W, axis=0).T.astype(jnp.float32)

    def one_pole(carry, inputs):
        factor, diag_inv, weight = inputs
        lower = factor.reshape(2, total, total) * keep[None]
        inverse = jnp.zeros((2, total, total), jnp.float32)
        last = (NS - 1) * W
        inverse = inverse.at[:, last:, last:].set(diag_inv[:, NS - 1])
        for step in range(NS - 2, -1, -1):
            start = step * W
            after = (step + 1) * W
            panel = lower[:, after:, start:start + W]
            block = inverse[:, after:, after:]
            row_part = -cdot_t(panel, block)
            inverse = inverse.at[:, start:start + W, after:].set(row_part)
            column = jnp.swapaxes(row_part, 1, 2)
            inverse = inverse.at[:, after:, start:start + W].set(column)
            inverse = inverse.at[:, start:start + W, start:start + W].set(diag_inv[:, step] - cdot_t(panel, column))
        return carry + weight[0] * inverse[0] - weight[1] * inverse[1], None

    summed, unused = lax.scan(one_pole, jnp.zeros((total, total), jnp.float32), (l_factor, dinv, weights))
    return summed.reshape(NS, N_ROW, W // N_ROW, NS, W)
```

```python
import jax
import jax.numpy as jnp
from jax import lax
from jax.sharding import PartitionSpec as P

PRECISION = lax.Precision.HIGH


def product(panel, values, part_cols):
    dims = (((1,), (0,)), ((), ()))

    def single(right):
        return lax.dot_general(
            panel, right, dims, precision=PRECISION, preferred_element_type=jnp.float32
        )

    by_real = single(values[0])
    by_imag = single(values[1])
    real = by_real[:, :part_cols] - by_imag[:, part_cols:]
    imag = by_imag[:, :part_cols] + by_real[:, part_cols:]
    return jnp.stack([real, imag], axis=1)


def sum_own_rows(partial_value, nrow, row_index):
    grouped = partial_value.reshape((nrow, -1) + partial_value.shape[1:])
    total = lax.dynamic_index_in_dim(grouped, row_index, 0, keepdims=False)
    for shift in range(1, nrow):
        target = lax.rem(row_index + shift, nrow)
        sent = lax.dynamic_index_in_dim(grouped, target, 0, keepdims=False)
        pairs = [(source, (source + shift) % nrow) for source in range(nrow)]
        total = total + lax.ppermute(sent, "row", pairs)
    return total


def on_device(l_factor, dinv, weights, tiles):
    nrow = lax.axis_size("row")
    ncol = lax.axis_size("col")
    npole = lax.axis_size("pole")
    row_index = lax.axis_index("row")
    col_index = lax.axis_index("col")
    factor = l_factor[0]
    diag_inv = dinv[0]
    weight = weights[0]
    nsup = factor.shape[1]
    rows_here = factor.shape[2]
    cols_here = factor.shape[4]
    width = rows_here * nrow
    per_row = ncol // nrow
    assert ncol == per_row * nrow
    tile_rows = nsup * width // tiles.shape[1]
    expanded = jnp.repeat(tiles.reshape(nsup, nsup, -1), tile_rows, axis=2)
    local_keep = lax.dynamic_slice_in_dim(expanded, row_index * rows_here, rows_here, 2)
    keep = local_keep.astype(jnp.float32)

    def weigh(values):
        return weight[0] * values[0] - weight[1] * values[1]

    panels = {}
    for step in range(nsup - 2, -1, -1):
        part = factor[:, step + 1 :, :, step, :] * keep[step, step + 1 :, :, None][None]
        flat = jnp.concatenate([part[0], part[1]], axis=2)
        flat = flat.reshape(-1, 2 * cols_here)
        panels[step] = lax.all_gather(flat, "col", axis=0, tiled=False)

    last = nsup - 1
    held = [diag_inv[0, last], diag_inv[1, last]]
    out = [[None] * nsup for _ in range(nsup)]
    newest_row = None
    for step in range(nsup - 2, -1, -1):
        span = nsup - 1 - step
        panel = panels[step]
        if newest_row is None:
            partial_value = -product(panel, held, cols_here)
        else:
            diag, row_block, column = newest_row
            front, rest = panel[:, :rows_here], panel[:, rows_here:]
            early = product(rest, held, cols_here)
            right = early + product(front, row_block, cols_here)
            new_column = [jnp.concatenate([diag[q], column[q]], axis=0) for q in (0, 1)]
            left = product(panel, new_column, cols_here)
            partial_value = -jnp.concatenate([left, right], axis=3)
            held = [
                jnp.concatenate(
                    [
                        new_column[q],
                        jnp.concatenate([row_block[q], held[q]], axis=0),
                    ],
                    axis=1,
                )
                for q in (0, 1)
            ]
        mine = sum_own_rows(partial_value, nrow, row_index)
        row_block = [mine[:, q].reshape(rows_here, span * cols_here) for q in (0, 1)]
        pieces = []
        inner = lax.rem(col_index, per_row)
        for shift in range(per_row):
            sent = lax.dynamic_index_in_dim(
                mine, lax.rem(inner + shift, per_row), 0, keepdims=False
            )
            pairs = []
            for row in range(nrow):
                for col in range(ncol):
                    target_row = col // per_row
                    target_col = row * per_row + (col % per_row + shift) % per_row
                    pairs.append((row * ncol + col, target_row * ncol + target_col))
            pieces.append(lax.ppermute(sent, ("row", "col"), pairs))
        ordered = [
            lax.select_n(lax.rem(inner - place + per_row, per_row), *pieces)
            if per_row > 1
            else pieces[0]
            for place in range(per_row)
        ]
        stacked = jnp.stack(
            [piece.reshape(2, cols_here, span, cols_here) for piece in ordered], axis=0
        )
        column = jnp.transpose(stacked, (1, 3, 0, 4, 2)).reshape(2, span * rows_here, cols_here)
        correction = product(panel, column, cols_here)
        share = sum_own_rows(correction, nrow, row_index)
        diag = [
            diag_inv[q, step] - share[:, q].reshape(rows_here, cols_here) for q in (0, 1)
        ]
        newest_row = (diag, row_block, column)
        pending = [weigh(row_block), weigh(diag)]
        tall = weigh(column).reshape(span, rows_here, cols_here)
        pending += [tall[place] for place in range(span)]
        if step == nsup - 2:
            pending.append(weigh([diag_inv[0, last], diag_inv[1, last]]))
        joined = jnp.concatenate(pending, axis=1)
        summed = lax.psum_scatter(joined, "pole", scatter_dimension=0, tiled=True)
        blocks = [
            summed[:, place * cols_here : (place + 1) * cols_here]
            for place in range(summed.shape[1] // cols_here)
        ]
        for place in range(span):
            out[step][step + 1 + place] = blocks[place]
            out[step + 1 + place][step] = blocks[span + 1 + place]
        out[step][step] = blocks[span]
        if step == nsup - 2:
            out[last][last] = blocks[-1]
    density = jnp.stack([jnp.stack(line, axis=1) for line in out], axis=0)
    return density.reshape(nsup, 1, rows_here // npole, nsup, cols_here)


def solution(mesh):
    return jax.shard_map(
        on_device,
        mesh=mesh,
        in_specs=(
            P("pole", None, None, "row", None, "col"),
            P("pole", None, None, "row", "col"),
            P("pole", None),
            P(),
        ),
        out_specs=P(None, "row", "pole", None, "col"),
        check_vma=False,
    )
```
